256 devices in a mesh: grp: 2 (over y), date: 16 (over z), row: 4 (over x), band: 2 (over core).
Axes of the slice: x: 4, y: 2, z: 16, core: 2. Of those that a mesh axis runs over, the one named last changes fastest.
The devices are a block of a 4x16x16 slice.
Arguments:
- reflect: bfloat16 [256, 6, 512, 1024], P('date', 'band', ('grp', 'row')), parts along dimension 2, may hold values from 0 to 0.59765625
- quality: int32 [256, 512, 1024], P('date', ('grp', 'row')), parts along dimension 1, may hold values from 0 to 1073741823
- instrument_ids: int32 [512], P(('grp', 'date')), parts along dimension 0, may hold values from 0 to 2
- day_of_year: int32 [512], P(('grp', 'date')), parts along dimension 0, may hold values from 1 to 365
- image_rank_values: int32 [512], P(('grp', 'date')), parts along dimension 0, may hold values from 0 to 63
- cloud_penalty: int32 [512], P(('grp', 'date')), parts along dimension 0, may hold values from 8 to 32
Outputs:
- composite: bfloat16 [6, 512, 1024], P('band', ('grp', 'row')), parts along dimension 1
- best_date: int32 [512, 1024], P(('grp', 'row')), parts along dimension 0
The draws below stay inside these ranges and needn't reach their ends.
There are 2 independent parts, one for each index of `grp`. The reference program is written for one: setup_inputs(seed, part) draws one part's arguments, and reference() takes and returns one part's arrays. A program takes and returns all parts, laid end to end along the dimension named above; each array names one. Nothing has to cross between parts.
All inputs are finite; a program needn't handle non-finite values.
Results may differ from the reference program's by a relative error of at most 0.001.
Values may be sent and summed in bfloat16 or wider, within the bound.
No kernel may reach another device: no remote copies, remote signals or barrier semaphores. Data moves between devices by JAX's collectives and lax.ppermute only.
A program may use at most 64 MiB of HBM per device.

```python
import jax
import jax.numpy as jnp
from jax import lax

BANDS = 6
COLS = 1024
RADIUS = 4
NDATE = 256
ROWS = 256


blob_count = 5


cell_grid = 8


def cloud_level(distance, reach):
    core = distance < reach
    edge = distance < 2 * reach
    return jnp.where(core, 3, jnp.where(edge, 2, 0)).astype(jnp.int32)


def draw_quality(key, part):
    stretch = max(1, COLS // ROWS)
    fixed_key = jax.random.fold_in(key, 17)
    spot_row = jax.random.randint(jax.random.fold_in(fixed_key, 1), (), 0, ROWS, dtype=jnp.int32)
    spot_col = jax.random.randint(jax.random.fold_in(fixed_key, 2), (), 0, COLS, dtype=jnp.int32)
    spot_reach = max(2, COLS // 6)
    rows_at = jnp.arange(ROWS, dtype=jnp.int32)[:, None]
    cols_at = jnp.arange(COLS, dtype=jnp.int32)[None, :]
    row_cell = rows_at * cell_grid // ROWS
    col_cell = cols_at * cell_grid // COLS

    def one_date(index):
        date_key = jax.random.fold_in(key, 1000 + index)
        keys = jax.random.split(date_key, 9)
        words = jax.random.randint(keys[0], (ROWS, COLS), 0, 1073741824, dtype=jnp.int32)
        words = words - (words & 3840)
        cell_rate = jax.random.randint(keys[1], (cell_grid, cell_grid), 0, 91, dtype=jnp.int32)
        rate = cell_rate[row_cell, col_cell]
        hazed = jax.random.randint(keys[2], (ROWS, COLS), 0, 100, dtype=jnp.int32) < rate
        level = jax.random.randint(keys[8], (ROWS, COLS), 1, 4, dtype=jnp.int32)
        faint = jnp.where(hazed, level, 0).astype(jnp.int32)
        centre_row = jax.random.randint(keys[3], (blob_count,), 0, ROWS, dtype=jnp.int32)
        centre_col = jax.random.randint(keys[4], (blob_count,), 0, COLS, dtype=jnp.int32)
        reach = jax.random.randint(keys[5], (blob_count,), 1, max(2, COLS // 4) + 1, dtype=jnp.int32)
        active = jax.random.randint(keys[6], (blob_count,), 0, 2, dtype=jnp.int32)
        persist = (jax.random.randint(keys[7], (), 0, 100, dtype=jnp.int32) < 92).astype(jnp.int32)
        cloud = faint
        shadow = jnp.zeros((ROWS, COLS), jnp.int32)
        for blob in range(blob_count + 1):
            if blob < blob_count:
                middle_row = centre_row[blob]
                middle_col = centre_col[blob]
                radius = reach[blob]
                live = active[blob]
            else:
                middle_row = spot_row
                middle_col = spot_col
                radius = jnp.int32(spot_reach)
                live = persist
            squared = radius * radius * live
            row_gap = (rows_at - middle_row) * stretch
            col_gap = cols_at - middle_col
            distance = row_gap * row_gap + col_gap * col_gap
            cloud = jnp.maximum(cloud, cloud_level(distance, squared))
            shade_row = (rows_at - middle_row - radius // stretch - 1) * stretch
            shade_col = cols_at - middle_col - radius
            shade_distance = shade_row * shade_row + shade_col * shade_col
            shadow = jnp.maximum(shadow, jnp.where(shade_distance < squared, 2 + (4 * shade_distance < squared), 0).astype(jnp.int32))
        return words + cloud * 256 + shadow * 1024
    return lax.map(one_date, jnp.arange(NDATE, dtype=jnp.int32))


def plant(array, stream_key, low, largest):
    shape = array.shape
    index_at = [jax.random.randint(jax.random.fold_in(stream_key, axis), (), 0, shape[axis]) for axis in range(len(shape))]
    array = array.at[tuple(index_at)].set(low)
    longest = shape.index(max(shape))
    index_at[longest] = (index_at[longest] + 1) % shape[longest]
    return array.at[tuple(index_at)].set(largest)


def block_levels(own_key, shape, cuts, low, high):
    def one(axis_at, shards_of):
        heights = jax.random.uniform(jax.random.fold_in(jax.random.fold_in(own_key, 6), axis_at), (shards_of,), jnp.float32, low / len(cuts), high / len(cuts))
        return jnp.repeat(jnp.exp(heights), shape[axis_at] // shards_of).reshape((-1,) + (1,) * (len(shape) - axis_at - 1))

    loudness = one(*cuts[0])
    for cut in cuts[1:]:
        loudness = loudness * one(*cut)
    return loudness


def setup_inputs(seed: int = 0, part: int = 0) -> dict:
    streams_of = jax.random.split(jax.random.key(seed), 7)
    part_keys = jax.random.split(jax.random.fold_in(streams_of[6], part), 7)
    return {
        "reflect": jnp.clip(0.59765625 * jax.random.uniform(part_keys[0], (NDATE, BANDS, ROWS, COLS), jnp.float32) ** block_levels(part_keys[0], (NDATE, BANDS, ROWS, COLS), ((0, 16), (1, 2), (2, 4)), -0.2, 0.2), 0.0, 0.59765625).astype(jnp.bfloat16),
        "quality": draw_quality(jax.random.fold_in(jax.random.fold_in(streams_of[6], part), 71), part),
        "instrument_ids": plant(jax.random.randint(part_keys[2], (NDATE,), 0, 3), jax.random.fold_in(part_keys[2], 1), 0, 2).astype(jnp.int32),
        "day_of_year": plant(jax.random.randint(part_keys[3], (NDATE,), 1, 366), jax.random.fold_in(part_keys[3], 1), 1, 365).astype(jnp.int32),
        "image_rank_values": plant(jax.random.randint(part_keys[4], (NDATE,), 0, 64), jax.random.fold_in(part_keys[4], 1), 0, 63).astype(jnp.int32),
        "cloud_penalty": plant(jax.random.randint(part_keys[5], (NDATE,), 8, 33), jax.random.fold_in(part_keys[5], 1), 8, 32).astype(jnp.int32),
    }


def haze_closeness_map(blocked_marker):
    padded = jnp.pad(blocked_marker, RADIUS)
    across = jnp.zeros((ROWS + 2 * RADIUS, COLS), jnp.int32)
    for shift in range(-RADIUS, RADIUS + 1):
        across = across + (RADIUS + 1 - abs(shift)) * padded[:, RADIUS + shift:RADIUS + shift + COLS]
    result = jnp.zeros((ROWS, COLS), jnp.int32)
    for shift in range(-RADIUS, RADIUS + 1):
        result = result + (RADIUS + 1 - abs(shift)) * across[RADIUS + shift:RADIUS + shift + ROWS]
    return result


def reference(reflect, quality, instrument_ids, day_of_year, image_rank_values, cloud_penalty):
    def step(carry, items):
        best_score, best_when, best_vals = carry
        image, words, blocker_type, doy, scaling_multiplier, deduction_amount, when = items
        blocked_marker = (jnp.right_shift(words, 8) & 3) + (jnp.right_shift(words, 10) & 3)
        closeness = haze_closeness_map(blocked_marker)
        apart = jnp.abs(doy - 196)
        yearly_cycle_part = jnp.minimum(apart, 365 - apart)
        merit_extra = jnp.where(blocker_type == 1, 300, jnp.where(blocker_type == 2, 500, 0)).astype(jnp.int32)
        cell_merit = 16 * scaling_multiplier + merit_extra - 4 * yearly_cycle_part - deduction_amount * closeness
        better = cell_merit >= best_score
        best_score = jnp.where(better, cell_merit, best_score)
        best_when = jnp.where(better, when, best_when)
        best_vals = jnp.where(better[None], image, best_vals)
        return (best_score, best_when, best_vals), None

    start = (jnp.full((ROWS, COLS), -(2 ** 30), jnp.int32), jnp.zeros((ROWS, COLS), jnp.int32),
             jnp.zeros((BANDS, ROWS, COLS), reflect.dtype))
    dates = jnp.arange(NDATE, dtype=jnp.int32)
    (best_score, best_when, best_vals), unused = lax.scan(
        step, start, (reflect, quality, instrument_ids, day_of_year, image_rank_values, cloud_penalty, dates))
    return best_vals, best_when
```

```python
import jax
import jax.numpy as jnp
from jax import lax
from jax.experimental import pallas as pl
from jax.experimental.pallas import tpu as pltpu
from jax.sharding import PartitionSpec as P

RADIUS = 4
TILE = 8
GROUP = 4
BLOCK = 256
F32 = jnp.float32
BF16 = jnp.bfloat16
I32 = jnp.int32


def tent(distance):
    return jnp.maximum(RADIUS + 1 - jnp.abs(distance), 0)


def iotas(shape):
    return lax.broadcasted_iota(I32, shape, 0), lax.broadcasted_iota(I32, shape, 1)


def obstruction(words):
    level = ((words >> 8) & 3) + ((words >> 10) & 3)
    return level.astype(F32)


def column_pass(blocked):
    cols = blocked.shape[1]
    side = BLOCK // 2
    k, n = iotas((2 * BLOCK, BLOCK))
    band = tent(k - side - n).astype(F32).astype(BF16)
    out = []
    for start in range(0, cols, BLOCK):
        low = max(0, start - side)
        high = min(cols, start + BLOCK + side)
        first = low - (start - side)
        part = jnp.dot(blocked[:, low:high], band[first : first + high - low], preferred_element_type=F32)
        out.append(part.astype(BF16))
    return jnp.concatenate(out, axis=1)


def terms(ids, days, ranks, penalties, t, dates):
    apart = jnp.abs(days[t] - 196)
    season = jnp.minimum(apart, 365 - apart)
    bonus = jnp.where(ids[t] == 1, 300, jnp.where(ids[t] == 2, 500, 0))
    fixed = 16 * ranks[t] + bonus - 4 * season
    return (fixed * dates + t).astype(F32), (penalties[t] * dates).astype(F32)


def edge_kernel(core, words, out):
    dates = words.shape[0]
    level = obstruction(words[...]).reshape(dates * TILE, -1).astype(BF16)
    row, col = iotas((dates * RADIUS, dates * TILE))
    wanted = (row // RADIUS) * TILE + row % RADIUS + (TILE - RADIUS) * core[0]
    pick = (wanted == col).astype(F32).astype(BF16)
    edge = jnp.dot(pick, level, preferred_element_type=F32).astype(BF16)
    out[...] = column_pass(edge)


def inner_kernel(core, ids, days, ranks, penalties, *refs):
    tiles, (keys, edge) = refs[:-2], refs[-2:]
    step = pl.program_id(0)
    group = tiles[0].shape[0]
    rows = keys.shape[0]
    dates = group * pl.num_programs(0)
    level = jnp.concatenate([obstruction(t[...]).reshape(group * TILE, -1) for t in tiles], axis=0)
    across = column_pass(level.astype(BF16))
    m, k = iotas((group * rows, across.shape[0]))
    same = (m // rows) == (k // TILE) % group
    gap = (k // (group * TILE)) * TILE + k % TILE - TILE * core[0] - m % rows
    mix = jnp.where(same, tent(gap), 0).astype(F32).astype(BF16)
    closeness = jnp.dot(mix, across, preferred_element_type=F32)
    best = None
    for i in range(group):
        own = closeness[i * rows : (i + 1) * rows]
        edge[i] = jnp.where(core[0] == 0, own[:TILE], own[rows - TILE :])
        base, slope = terms(ids, days, ranks, penalties, step * group + i, dates)
        key = base - slope * own
        best = key if best is None else jnp.maximum(best, key)

    @pl.when(step == 0)
    def _():
        keys[...] = best

    @pl.when(step > 0)
    def _():
        keys[...] = jnp.maximum(keys[...], best)


def outer_kernel(place, ids, days, ranks, penalties, keys, edge, halo, out):
    core, own = place[0], place[1]
    dates = edge.shape[0]
    rows = keys.shape[0]
    m, k = iotas((dates * TILE, dates * RADIUS))
    same = (m // TILE) == (k // RADIUS)
    gap = k % RADIUS - m % TILE - RADIUS + (RADIUS + TILE) * core
    mix = jnp.where(same, tent(gap), 0).astype(F32).astype(BF16)
    rest = jnp.dot(mix, halo[...], preferred_element_type=F32)
    best = None
    for t in range(dates):
        base, slope = terms(ids, days, ranks, penalties, t, dates)
        key = base - slope * (edge[t] + rest[t * TILE : (t + 1) * TILE])
        best = key if best is None else jnp.maximum(best, key)
    low_tile, high_tile = (0, rows // TILE - 1)
    across = keys.shape[1] // BLOCK
    ndate = dates * place[2]
    for i in range(rows // TILE):
        key = keys[i * TILE : (i + 1) * TILE]
        if i == low_tile:
            key = jnp.where(core == 0, best, key)
        if i == high_tile:
            key = jnp.where(core == 0, key, best)
        key = key.astype(I32)
        when = key & (dates - 1)
        score = (key - when) // dates
        full = score * ndate + (own * dates + when)
        for j in range(across):
            out[i * across + j] = full[:, j * BLOCK : (j + 1) * BLOCK]


def choose_kernel(keys, reflect, out):
    dates = reflect.shape[0]
    for j in range(keys.shape[1]):
        when = keys[0, j] & (dates - 1)
        hits = [when == t for t in range(1, dates)]
        for k in range(reflect.shape[1]):
            at = (k, slice(None), slice(j * BLOCK, (j + 1) * BLOCK))
            value = reflect[(0, *at)].astype(F32)
            for t in range(1, dates):
                value = jnp.where(hits[t - 1], reflect[(t, *at)].astype(F32), value)
            out[0, j, k, 0] = value.astype(BF16)


def winner_kernel(count, keys, out):
    best = keys[0]
    for s in range(1, keys.shape[0]):
        best = jnp.maximum(best, keys[s])
    out[...] = best & (count[0] - 1)


def merge_kernel(dates, when, values, out):
    sources, bands, halves = values.shape[:3]
    for h in range(halves):
        date = when[h]
        hits = [date >= s * dates[0] for s in range(1, sources)]
        for k in range(bands):
            value = values[0, k, h].astype(F32)
            for s in range(1, sources):
                value = jnp.where(hits[s - 1], values[s, k, h].astype(F32), value)
            out[k, h] = value.astype(BF16)
        out[bands, h] = date.astype(F32).astype(BF16)


def spread_kernel(parts, composite, best):
    sources, groups, halves = parts.shape[:3]
    across = best.shape[1] // BLOCK
    half = best.shape[0] // halves
    for s in range(sources):
        cols = slice((s % across) * BLOCK, (s % across + 1) * BLOCK)
        for h in range(halves):
            top = h * half + (s // across) * TILE
            rows = slice(top, top + TILE)
            for k in range(groups - 1):
                composite[k, rows, cols] = parts[s, k, h]
            best[rows, cols] = parts[s, groups - 1, h].astype(F32).astype(I32)


def per_device(reflect, quality, instrument_ids, day_of_year, image_rank_values, cloud_penalty):
    dates, rows, cols = quality.shape
    bands = reflect.shape[1]
    sources, chips, cores = (lax.axis_size(a) for a in ("date", "row", "band"))
    own, core = lax.axis_index("date"), lax.axis_index("band")
    half = rows // cores
    shape = jax.ShapeDtypeStruct
    smem = pl.BlockSpec(memory_space=pltpu.SMEM)
    vmem = pl.BlockSpec(memory_space=pltpu.VMEM)
    scenes = (instrument_ids, day_of_year, image_rank_values, cloud_penalty)
    core_at = core.astype(I32)[None]

    edge_rows = pl.pallas_call(
        edge_kernel,
        out_shape=shape((dates * RADIUS, cols), BF16),
        grid_spec=pltpu.PrefetchScalarGridSpec(
            num_scalar_prefetch=1,
            grid=(1,),
            in_specs=[pl.BlockSpec((dates, TILE, cols), lambda g, c: (0, c[0] * (rows // TILE - 1), 0))],
            out_specs=pl.BlockSpec((dates * RADIUS, cols), lambda g, c: (0, 0)),
        ),
        name="edge",
    )(core_at, quality)
    links = []
    for x in range(chips - 1):
        links += [(x * cores + 1, (x + 1) * cores), ((x + 1) * cores, x * cores + 1)]
    halo = lax.ppermute(edge_rows, ("row", "band"), links)

    ntile = half // TILE + 1
    inner_keys, edge_part = pl.pallas_call(
        inner_kernel,
        out_shape=(shape((half, cols), F32), shape((dates, TILE, cols), F32)),
        grid_spec=pltpu.PrefetchScalarGridSpec(
            num_scalar_prefetch=5,
            grid=(dates // GROUP,),
            in_specs=[
                pl.BlockSpec((GROUP, TILE, cols), lambda g, c, *_, i=i: (g, c[0] * (ntile - 2) + i, 0)) for i in range(ntile)
            ],
            out_specs=(
                pl.BlockSpec((half, cols), lambda g, *_: (0, 0)),
                pl.BlockSpec((GROUP, TILE, cols), lambda g, *_: (g, 0, 0)),
            ),
        ),
        name="inner",
    )(core_at, *scenes, *([quality] * ntile))

    place = jnp.stack([core, own, jnp.int32(sources)]).astype(I32)
    keys = pl.pallas_call(
        outer_kernel,
        out_shape=shape((sources, TILE, BLOCK), I32),
        in_specs=[smem] * 5 + [vmem] * 3,
        out_specs=vmem,
        name="outer",
    )(place, *scenes, inner_keys, edge_part, halo)

    arrived = lax.all_to_all(keys, "date", 0, 0, tiled=True)
    both = lax.all_gather(keys, "band")

    across = cols // BLOCK
    down = half // TILE
    values = pl.pallas_call(
        choose_kernel,
        out_shape=shape((down, across, bands, cores, TILE, BLOCK), BF16),
        grid=(rows // TILE,),
        in_specs=[
            pl.BlockSpec((1, across, TILE, BLOCK), lambda i: (i // down, i % down, 0, 0)),
            pl.BlockSpec((dates, bands, TILE, cols), lambda i: (0, 0, i, 0)),
        ],
        out_specs=pl.BlockSpec((1, across, bands, 1, TILE, BLOCK), lambda i: (i % down, 0, 0, i // down, 0, 0)),
        name="choose",
    )(both, reflect)
    values = values.reshape(sources, bands * cores * TILE, BLOCK)
    values = lax.all_to_all(values, "date", 0, 0, tiled=True)
    values = values.reshape(sources, bands, cores, TILE, BLOCK)

    won = pl.pallas_call(
        winner_kernel,
        out_shape=shape((TILE, BLOCK), I32),
        in_specs=[smem, vmem],
        out_specs=vmem,
        name="winner",
    )(jnp.full((1,), dates * sources, I32), arrived)
    won = lax.all_gather(won, "band")

    part = pl.pallas_call(
        merge_kernel,
        out_shape=shape((bands + 1, cores, TILE, BLOCK), BF16),
        in_specs=[smem, vmem, vmem],
        out_specs=vmem,
        name="merge",
    )(jnp.full((1,), dates, I32), won, values)
    parts = lax.all_gather(part.reshape((bands + 1) * cores * TILE, BLOCK), "date")
    return pl.pallas_call(
        spread_kernel,
        out_shape=(shape((bands, rows, cols), BF16), shape((rows, cols), I32)),
        in_specs=[vmem],
        out_specs=(vmem, vmem),
        name="spread",
    )(parts.reshape(sources, bands + 1, cores, TILE, BLOCK))


def solution(mesh):
    placed = (
        P("date", "band", ("grp", "row"), None),
        P("date", ("grp", "row"), None),
        P(("grp", "date")),
        P(("grp", "date")),
        P(("grp", "date")),
        P(("grp", "date")),
    )
    return jax.shard_map(
        per_device,
        mesh=mesh,
        in_specs=placed,
        out_specs=(P("band", ("grp", "row"), None), P(("grp", "row"), None)),
        check_vma=False,
    )
```

```python
import functools

import jax
import jax.numpy as jnp
from jax import lax
from jax.experimental import pallas as pl
from jax.experimental.pallas import tpu as pltpu
from jax.sharding import PartitionSpec as P

RADIUS = 4
TILE = 8
GROUP = 4
BLOCK = 256
FLOOR = 126 * 1024
BIG = 57
F32 = jnp.float32
BF16 = jnp.bfloat16
I32 = jnp.int32


def tent(distance):
    return jnp.maximum(RADIUS + 1 - jnp.abs(distance), 0)


def iotas(shape):
    return lax.broadcasted_iota(I32, shape, 0), lax.broadcasted_iota(I32, shape, 1)


def obstruction(words):
    level = ((words >> 8) & 3) + ((words >> 10) & 3)
    return level.astype(F32)


def column_pass(blocked):
    cols = blocked.shape[1]
    side = BLOCK // 2
    k, n = iotas((2 * BLOCK, BLOCK))
    band = tent(k - side - n).astype(F32).astype(BF16)
    out = []
    for start in range(0, cols, BLOCK):
        low = max(0, start - side)
        high = min(cols, start + BLOCK + side)
        first = low - (start - side)
        part = jnp.dot(blocked[:, low:high], band[first : first + high - low], preferred_element_type=F32)
        out.append(part.astype(BF16))
    return jnp.concatenate(out, axis=1)


def terms(ids, days, ranks, penalties, t, dates):
    apart = jnp.abs(days[t] - 196)
    season = jnp.minimum(apart, 365 - apart)
    bonus = jnp.where(ids[t] == 1, 300, jnp.where(ids[t] == 2, 500, 0))
    fixed = 16 * ranks[t] + bonus - 4 * season
    return (fixed * dates + t).astype(F32), (penalties[t] * dates).astype(F32)


def fetches(source, target, sems, cuts):
    copies = [pltpu.make_async_copy(source.at[src], target.at[dst], sems.at[i]) for i, (src, dst) in enumerate(cuts)]
    for copy in copies:
        copy.start()
    return copies


def edge_kernel(words, first, last, near, sems):
    dates, rows, _ = words.shape
    row, col = iotas((dates * RADIUS, dates * TILE))
    whole = slice(None)
    cuts = [((whole, pl.ds(start, TILE)), side) for side, start in enumerate((0, rows - TILE))]
    copies = fetches(words, near, sems, cuts)
    for side, (out, shift) in enumerate(((first, 0), (last, TILE - RADIUS))):
        wanted = (row // RADIUS) * TILE + row % RADIUS + shift
        pick = (wanted == col).astype(F32).astype(BF16)
        copies[side].wait()
        level = obstruction(near[side]).reshape(dates * TILE, -1).astype(BF16)
        edge = jnp.dot(pick, level, preferred_element_type=F32).astype(BF16)
        out[...] = column_pass(edge)


def inner_kernel(ids, days, ranks, penalties, words, keys, edge, near, sems):
    dates, rows, cols = words.shape
    copies = fetches(words, near, sems, [(pl.ds(t, GROUP), pl.ds(t, GROUP)) for t in range(0, dates, GROUP)])
    m, k = iotas((GROUP * rows, GROUP * rows))
    mix = jnp.where(m // rows == k // rows, tent(k % rows - m % rows), 0).astype(F32).astype(BF16)
    for step, copy in enumerate(copies):
        copy.wait()
        level = obstruction(near[step * GROUP : (step + 1) * GROUP]).reshape(GROUP * rows, cols).astype(BF16)
        across = column_pass(level)
        closeness = jnp.dot(mix, across, preferred_element_type=F32)
        best = None
        for i in range(GROUP):
            t = step * GROUP + i
            own = closeness[i * rows : (i + 1) * rows]
            edge[t, 0] = own[:TILE]
            edge[t, 1] = own[rows - TILE :]
            base, slope = terms(ids, days, ranks, penalties, t, dates)
            key = base - slope * own
            best = key if best is None else jnp.maximum(best, key)
        keys[...] = best if step == 0 else jnp.maximum(keys[...], best)


def small(value):
    return value.astype(F32).astype(BF16)


def coded(number):
    power = jnp.full(number.shape, 2.0**-32, F32)
    for bit in range(6):
        power = power * jnp.where(number & (1 << (7 + bit)) != 0, 2.0 ** (1 << bit), 1.0)
    return (((number & 127) + 128).astype(F32) * power).astype(BF16)


def pick_kernel(ids, days, ranks, penalties, keys, edge, above, below, reflect, out, near, sems):
    dates, bands, rows, cols = reflect.shape
    across = cols // BLOCK
    tall = rows * across // out.shape[0]
    whole = slice(None)
    cuts = [(whole, whole, pl.ds(row, tall)) for row in range(0, rows, tall)]
    copies = fetches(reflect, near, sems, [(cut, cut) for cut in cuts])
    m, k = iotas((dates * TILE, dates * RADIUS))
    same = m // TILE == k // RADIUS
    pairs = [terms(ids, days, ranks, penalties, t, dates) for t in range(dates)]
    ends = []
    for side, halo, shift in ((0, above, -RADIUS), (1, below, TILE)):
        mix = jnp.where(same, tent(k % RADIUS + shift - m % TILE), 0).astype(F32).astype(BF16)
        rest = jnp.dot(mix, halo[...], preferred_element_type=F32)
        best = None
        for t, (base, slope) in enumerate(pairs):
            key = base - slope * (edge[t, side] + rest[t * TILE : (t + 1) * TILE])
            best = key if best is None else jnp.maximum(best, key)
        ends.append(best)
    full = jnp.concatenate([ends[0], keys[TILE : rows - TILE], ends[1]], axis=0).astype(I32)
    full = full + FLOOR * dates
    when = small(full & (dates - 1))
    high = coded(full >> 8)
    low = small(full & 255)
    for i, copy in enumerate(copies):
        copy.wait()
        for j in range(across):
            at = (slice(i * tall, (i + 1) * tall), slice(j * BLOCK, (j + 1) * BLOCK))
            chosen = when[at]
            hits = [chosen == jnp.asarray(t, BF16) for t in range(dates)]
            owner = i * across + j
            for band in range(bands):
                value = near[(0, band, *at)]
                for t in range(1, dates):
                    value = jnp.where(hits[t], near[(t, band, *at)], value)
                out[owner, band * tall : (band + 1) * tall] = value
            out[owner, bands * tall : (bands + 1) * tall] = high[at]
            out[owner, (bands + 1) * tall : (bands + 2) * tall] = low[at]


def scored(low, dates):
    number = low.astype(F32).astype(I32)
    return small(number - (number & (dates - 1)))


def merge_kernel(dates, arrived, out):
    sources, groups, tall, _ = arrived.shape
    bands = groups - 2
    high, low = arrived[0, bands], arrived[0, bands + 1]
    floor = scored(low, dates)
    source = jnp.zeros(high.shape, BF16)
    values = [arrived[0, k] for k in range(bands)]
    for s in range(1, sources):
        h, l = arrived[s, bands], arrived[s, bands + 1]
        better = (h > high) | ((h == high) & (l >= floor))
        high, low = jnp.where(better, h, high), jnp.where(better, l, low)
        floor = jnp.where(better, scored(l, dates), floor)
        source = jnp.where(better, jnp.asarray(s, BF16), source)
        values = [jnp.where(better, arrived[s, k], v) for k, v in enumerate(values)]
    when = low.astype(F32).astype(I32) & (dates - 1)
    date = source.astype(F32) * dates + when.astype(F32)
    parts = [*values, date.astype(BF16)]
    for d in range(sources):
        for k, part in enumerate(parts):
            out[d, k] = part


def spread_kernel(parts, composite, best):
    sources, groups, tall, wide = parts.shape
    across = best.shape[1] // wide
    for s in range(sources):
        rows = slice((s // across) * tall, (s // across + 1) * tall)
        cols = slice((s % across) * wide, (s % across + 1) * wide)
        for k in range(groups - 1):
            composite[k, rows, cols] = parts[s, k]
        best[rows, cols] = parts[s, groups - 1].astype(F32).astype(I32)


def per_device(reflect, quality, instrument_ids, day_of_year, image_rank_values, cloud_penalty):
    dates, rows, cols = quality.shape
    bands = reflect.shape[1]
    sources, chips = lax.axis_size("date"), lax.axis_size("row")
    across = cols // BLOCK
    down = sources // across
    tall = rows // down
    shape = jax.ShapeDtypeStruct
    smem = pl.BlockSpec(memory_space=pltpu.SMEM)
    vmem = pl.BlockSpec(memory_space=pltpu.VMEM)
    hbm = pl.BlockSpec(memory_space=pltpu.HBM)
    scenes = (instrument_ids, day_of_year, image_rank_values, cloud_penalty)

    def grant(mib):
        return pltpu.CompilerParams(vmem_limit_bytes=mib << 20)

    row_shape = shape((dates * RADIUS, cols), BF16)
    first, last = pl.pallas_call(
        edge_kernel,
        out_shape=(row_shape, row_shape),
        in_specs=[hbm],
        out_specs=(vmem, vmem),
        scratch_shapes=[pltpu.VMEM((2, dates, TILE, cols), I32), pltpu.SemaphoreType.DMA((2,))],
        compiler_params=grant(BIG),
        name="edge",
    )(quality)
    onward = [(x, x + 1) for x in range(chips - 1)]
    above = lax.ppermute(last, "row", onward)
    below = lax.ppermute(first, "row", [(j, i) for i, j in onward])

    inner_keys, edge_part = pl.pallas_call(
        inner_kernel,
        out_shape=(shape((rows, cols), F32), shape((dates, 2, TILE, cols), F32)),
        in_specs=[smem] * 4 + [hbm],
        out_specs=(vmem, vmem),
        scratch_shapes=[pltpu.VMEM((dates, rows, cols), I32), pltpu.SemaphoreType.DMA((dates // GROUP,))],
        compiler_params=grant(BIG),
        name="inner",
    )(*scenes, quality)

    packed = pl.pallas_call(
        pick_kernel,
        out_shape=shape((sources, (bands + 2) * tall, BLOCK), BF16),
        in_specs=[smem] * 4 + [vmem] * 4 + [hbm],
        out_specs=vmem,
        scratch_shapes=[pltpu.VMEM((dates, bands, rows, cols), BF16), pltpu.SemaphoreType.DMA((down,))],
        compiler_params=grant(BIG),
        name="pick",
    )(*scenes, inner_keys, edge_part, above, below, reflect)
    arrived = lax.all_to_all(packed, "date", 0, 0, tiled=True)
    part = pl.pallas_call(
        functools.partial(merge_kernel, dates),
        out_shape=shape((sources, bands + 1, tall, BLOCK), BF16),
        in_specs=[vmem],
        out_specs=vmem,
        compiler_params=grant(8),
        name="merge",
    )(arrived.reshape(sources, bands + 2, tall, BLOCK))
    parts = lax.all_to_all(part.reshape(sources, (bands + 1) * tall, BLOCK), "date", 0, 0, tiled=True)
    return pl.pallas_call(
        spread_kernel,
        out_shape=(shape((bands, rows, cols), BF16), shape((rows, cols), I32)),
        in_specs=[vmem],
        out_specs=(vmem, vmem),
        compiler_params=grant(8),
        name="spread",
    )(parts.reshape(sources, bands + 1, tall, BLOCK))


def solution(mesh):
    placed = (
        P("date", "band", ("grp", "row"), None),
        P("date", ("grp", "row"), None),
        P(("grp", "date")),
        P(("grp", "date")),
        P(("grp", "date")),
        P(("grp", "date")),
    )
    return jax.shard_map(
        per_device,
        mesh=mesh,
        in_specs=placed,
        out_specs=(P("band", ("grp", "row"), None), P(("grp", "row"), None)),
        check_vma=False,
    )
```

```python
import functools

import jax
import jax.numpy as jnp
from jax import lax
from jax.experimental import pallas as pl
from jax.experimental.pallas import tpu as pltpu
from jax.sharding import PartitionSpec as P

RADIUS = 4
TILE = 8
GROUP = 4
BLOCK = 256
FLOOR = 126 * 1024
BIG = 50
F32 = jnp.float32
BF16 = jnp.bfloat16
I32 = jnp.int32


def tent(distance):
    return jnp.maximum(RADIUS + 1 - jnp.abs(distance), 0)


def iotas(shape):
    return lax.broadcasted_iota(I32, shape, 0), lax.broadcasted_iota(I32, shape, 1)


def obstruction(words):
    level = ((words >> 8) & 3) + ((words >> 10) & 3)
    return level.astype(F32)


def column_pass(blocked):
    cols = blocked.shape[1]
    side = BLOCK // 2
    k, n = iotas((2 * BLOCK, BLOCK))
    band = tent(k - side - n).astype(F32).astype(BF16)
    out = []
    for start in range(0, cols, BLOCK):
        low = max(0, start - side)
        high = min(cols, start + BLOCK + side)
        first = low - (start - side)
        part = jnp.dot(blocked[:, low:high], band[first : first + high - low], preferred_element_type=F32)
        out.append(part.astype(BF16))
    return jnp.concatenate(out, axis=1)


def terms(ids, days, ranks, penalties):
    dates = ids.shape[0]
    apart = jnp.abs(days - 196)
    season = jnp.minimum(apart, 365 - apart)
    bonus = jnp.where(ids == 1, 300, jnp.where(ids == 2, 500, 0))
    fixed = (16 * ranks + bonus - 4 * season) * dates + jnp.arange(dates, dtype=I32)
    return jnp.concatenate([fixed, penalties * dates]).astype(F32)


def fetches(source, target, sems, cuts):
    copies = [pltpu.make_async_copy(source.at[src], target.at[dst], sems.at[i]) for i, (src, dst) in enumerate(cuts)]
    for copy in copies:
        copy.start()
    return copies


def edge_kernel(words, first, last, near, sems):
    dates, rows, _ = words.shape
    row, col = iotas((dates * RADIUS, dates * TILE))
    whole = slice(None)
    cuts = [((whole, pl.ds(start, TILE)), side) for side, start in enumerate((0, rows - TILE))]
    copies = fetches(words, near, sems, cuts)
    for side, (out, shift) in enumerate(((first, 0), (last, TILE - RADIUS))):
        wanted = (row // RADIUS) * TILE + row % RADIUS + shift
        pick = (wanted == col).astype(F32).astype(BF16)
        copies[side].wait()
        level = obstruction(near[side]).reshape(dates * TILE, -1).astype(BF16)
        edge = jnp.dot(pick, level, preferred_element_type=F32).astype(BF16)
        out[...] = column_pass(edge)


def inner_kernel(scenes, words, keys, edge, near, sems):
    dates, rows, cols = words.shape
    copies = fetches(words, near, sems, [(pl.ds(t, GROUP), pl.ds(t, GROUP)) for t in range(0, dates, GROUP)])
    m, k = iotas((GROUP * rows, GROUP * rows))
    mix = jnp.where(m // rows == k // rows, tent(k % rows - m % rows), 0).astype(F32).astype(BF16)
    for step, copy in enumerate(copies):
        copy.wait()
        level = obstruction(near[step * GROUP : (step + 1) * GROUP]).reshape(GROUP * rows, cols).astype(BF16)
        across = column_pass(level)
        closeness = jnp.dot(mix, across, preferred_element_type=F32)
        best = None
        for i in range(GROUP):
            t = step * GROUP + i
            own = closeness[i * rows : (i + 1) * rows]
            edge[t, 0] = own[:TILE]
            edge[t, 1] = own[rows - TILE :]
            base, slope = scenes[t], scenes[dates + t]
            key = base - slope * own
            best = key if best is None else jnp.maximum(best, key)
        keys[...] = best if step == 0 else jnp.maximum(keys[...], best)


def small(value):
    return value.astype(F32).astype(BF16)


def coded(number):
    power = jnp.full(number.shape, 2.0**-64, F32)
    for bit in range(7):
        power = power * jnp.where(number & (1 << (7 + bit)) != 0, 2.0 ** (1 << bit), 1.0)
    return (((number & 127) + 128).astype(F32) * power).astype(BF16)


def pick_kernel(own, scenes, keys, edge, above, below, reflect, keep, send, near, when, high, low, sems):
    dates, bands, rows, cols = reflect.shape
    across = cols // BLOCK
    tall = when.shape[0] * across // (2 * keep.shape[0])
    whole = slice(None)
    cuts = [(whole, whole, pl.ds(row, tall)) for row in range(0, rows, tall)]
    copies = fetches(reflect, near, sems, [(cut, cut) for cut in cuts])
    parity = own[0] & 1
    m, k = iotas((dates * TILE, dates * RADIUS))
    same = m // TILE == k // RADIUS
    pairs = [(scenes[t], scenes[dates + t]) for t in range(dates)]
    ends = []
    for side, halo, shift in ((0, above, -RADIUS), (1, below, TILE)):
        mix = jnp.where(same, tent(k % RADIUS + shift - m % TILE), 0).astype(F32).astype(BF16)
        rest = jnp.dot(mix, halo[...], preferred_element_type=F32)
        best = None
        for t, (base, slope) in enumerate(pairs):
            key = base - slope * (edge[t, side] + rest[t * TILE : (t + 1) * TILE])
            best = key if best is None else jnp.maximum(best, key)
        ends.append(best)
    full = jnp.concatenate([ends[0], keys[TILE : rows - TILE], ends[1]], axis=0).astype(I32)
    full = full + FLOOR * dates
    date = full & (dates - 1)
    score = (full - date) // dates
    when[...] = small(date)
    high[...] = coded(score >> 3)
    low[...] = small((score & 7) * (2 * dates) + (parity * dates + date))
    for i, copy in enumerate(copies):
        copy.wait()
        for j in range(across // 2):
            slot = i * (across // 2) + j
            for side, out in enumerate((keep, send)):
                col = pl.multiple_of((2 * j + (parity ^ side)) * BLOCK, BLOCK)
                at = (pl.ds(i * tall, tall), pl.ds(col, BLOCK))
                chosen = when[at]
                hits = [chosen == jnp.asarray(t, BF16) for t in range(dates)]
                for band in range(bands):
                    value = near[(0, band, *at)]
                    for t in range(1, dates):
                        value = jnp.where(hits[t], near[(t, band, *at)], value)
                    out[slot, band] = value
                out[slot, bands] = high[at]
                out[slot, bands + 1] = low[at]


def pair_kernel(mine, other, out):
    slots, groups = mine.shape[:2]
    bands = groups - 2
    for s in range(slots):
        high, low = mine[s, bands], mine[s, bands + 1]
        h, l = other[s, bands], other[s, bands + 1]
        better = (h > high) | ((h == high) & (l > low))
        for k in range(groups):
            out[s, k] = jnp.where(better, other[s, k], mine[s, k])


def scored(low, dates):
    number = low.astype(F32).astype(I32)
    return small(number - (number & (dates - 1)))


def merge_kernel(dates, arrived, out):
    sources, groups = arrived.shape[:2]
    bands = groups - 2
    high, low = arrived[0, bands], arrived[0, bands + 1]
    floor = scored(low, dates)
    source = jnp.zeros(high.shape, BF16)
    values = [arrived[0, k] for k in range(bands)]
    for s in range(1, sources):
        h, l = arrived[s, bands], arrived[s, bands + 1]
        better = (h > high) | ((h == high) & (l >= floor))
        high, low = jnp.where(better, h, high), jnp.where(better, l, low)
        floor = jnp.where(better, scored(l, dates), floor)
        source = jnp.where(better, jnp.asarray(s, BF16), source)
        values = [jnp.where(better, arrived[s, k], v) for k, v in enumerate(values)]
    when = low.astype(F32).astype(I32) & (dates - 1)
    date = source.astype(F32) * dates + when.astype(F32)
    parts = [*values, date.astype(BF16)]
    for d in range(sources):
        for k, part in enumerate(parts):
            out[d, k] = part


def spread_kernel(own, mine, other, composite, best):
    slots, groups, tall, wide = mine.shape
    across = best.shape[1] // wide
    even = (own[0] & 1) == 0
    for owner in range(2 * slots):
        rows = slice((owner // across) * tall, (owner // across + 1) * tall)
        cols = slice((owner % across) * wide, (owner % across + 1) * wide)
        here = even if owner % 2 == 0 else jnp.logical_not(even)
        for k in range(groups):
            part = jnp.where(here, mine[owner // 2, k], other[owner // 2, k])
            if k < groups - 1:
                composite[k, rows, cols] = part
            else:
                best[rows, cols] = part.astype(F32).astype(I32)


def per_device(reflect, quality, instrument_ids, day_of_year, image_rank_values, cloud_penalty):
    dates, rows, cols = quality.shape
    bands = reflect.shape[1]
    sources, chips = lax.axis_size("date"), lax.axis_size("row")
    own = lax.axis_index("date").astype(I32)[None]
    across = cols // BLOCK
    down = sources // across
    tall = rows // down
    shape = jax.ShapeDtypeStruct
    smem = pl.BlockSpec(memory_space=pltpu.SMEM)
    vmem = pl.BlockSpec(memory_space=pltpu.VMEM)
    hbm = pl.BlockSpec(memory_space=pltpu.HBM)
    scenes = terms(instrument_ids, day_of_year, image_rank_values, cloud_penalty)

    def grant(mib):
        return pltpu.CompilerParams(vmem_limit_bytes=mib << 20)

    row_shape = shape((dates * RADIUS, cols), BF16)
    first, last = pl.pallas_call(
        edge_kernel,
        out_shape=(row_shape, row_shape),
        in_specs=[hbm],
        out_specs=(vmem, vmem),
        scratch_shapes=[pltpu.VMEM((2, dates, TILE, cols), I32), pltpu.SemaphoreType.DMA((2,))],
        compiler_params=grant(BIG),
        name="edge",
    )(quality)
    onward = [(x, x + 1) for x in range(chips - 1)]
    above = lax.ppermute(last, "row", onward)
    below = lax.ppermute(first, "row", [(j, i) for i, j in onward])

    inner_keys, edge_part = pl.pallas_call(
        inner_kernel,
        out_shape=(shape((rows, cols), F32), shape((dates, 2, TILE, cols), F32)),
        in_specs=[smem, hbm],
        out_specs=(vmem, vmem),
        scratch_shapes=[pltpu.VMEM((dates, rows, cols), I32), pltpu.SemaphoreType.DMA((dates // GROUP,))],
        compiler_params=grant(BIG),
        name="inner",
    )(scenes, quality)

    slots = sources // 2
    packed = shape((slots, bands + 2, tall, BLOCK), BF16)
    plane = pltpu.VMEM((rows, cols), BF16)
    keep, send = pl.pallas_call(
        pick_kernel,
        out_shape=(packed, packed),
        in_specs=[smem] * 2 + [vmem] * 4 + [hbm],
        out_specs=(vmem, vmem),
        scratch_shapes=[
            pltpu.VMEM((dates, bands, rows, cols), BF16), plane, plane, plane, pltpu.SemaphoreType.DMA((down,))
        ],
        compiler_params=grant(BIG),
        name="pick",
    )(own, scenes, inner_keys, edge_part, above, below, reflect)
    swap = [(z, z ^ 1) for z in range(sources)]
    alike = [list(range(first, sources, 2)) for first in range(2)]

    def swapped(parts):
        return lax.ppermute(parts.reshape(-1, BLOCK), "date", swap).reshape(parts.shape)

    def spread_out(parts):
        flat = parts.reshape(parts.shape[0], -1, BLOCK)
        return lax.all_to_all(flat, "date", 0, 0, axis_index_groups=alike, tiled=True).reshape(parts.shape)

    paired = pl.pallas_call(
        pair_kernel,
        out_shape=packed,
        in_specs=[vmem, vmem],
        out_specs=vmem,
        compiler_params=grant(8),
        name="pair",
    )(keep, swapped(send))
    part = pl.pallas_call(
        functools.partial(merge_kernel, 2 * dates),
        out_shape=shape((slots, bands + 1, tall, BLOCK), BF16),
        in_specs=[vmem],
        out_specs=vmem,
        compiler_params=grant(8),
        name="merge",
    )(spread_out(paired))
    parts = spread_out(part)
    return pl.pallas_call(
        spread_kernel,
        out_shape=(shape((bands, rows, cols), BF16), shape((rows, cols), I32)),
        in_specs=[smem, vmem, vmem],
        out_specs=(vmem, vmem),
        compiler_params=grant(8),
        name="spread",
    )(own, parts, swapped(parts))


def solution(mesh):
    placed = (
        P("date", "band", ("grp", "row"), None),
        P("date", ("grp", "row"), None),
        P(("grp", "date")),
        P(("grp", "date")),
        P(("grp", "date")),
        P(("grp", "date")),
    )
    return jax.shard_map(
        per_device,
        mesh=mesh,
        in_specs=placed,
        out_specs=(P("band", ("grp", "row"), None), P(("grp", "row"), None)),
        check_vma=False,
    )
```

```python
import functools

import jax
import jax.numpy as jnp
from jax import lax
from jax.experimental import pallas as pl
from jax.experimental.pallas import tpu as pltpu
from jax.sharding import PartitionSpec as P

RADIUS = 4
TILE = 8
GROUP = 4
BLOCK = 256
LANES = 128
FLOOR = 126 * 1024
BIG = 50
F32 = jnp.float32
BF16 = jnp.bfloat16
I32 = jnp.int32


def tent(distance):
    return jnp.maximum(RADIUS + 1 - jnp.abs(distance), 0)


def iotas(shape):
    return lax.broadcasted_iota(I32, shape, 0), lax.broadcasted_iota(I32, shape, 1)


def obstruction(words):
    level = ((words >> 8) & 3) + ((words >> 10) & 3)
    return level.astype(F32)


def column_pass(blocked):
    cols = blocked.shape[1]
    side = BLOCK // 2
    k, n = iotas((2 * BLOCK, BLOCK))
    band = tent(k - side - n).astype(F32).astype(BF16)
    out = []
    for start in range(0, cols, BLOCK):
        low = max(0, start - side)
        high = min(cols, start + BLOCK + side)
        first = low - (start - side)
        part = jnp.dot(blocked[:, low:high], band[first : first + high - low], preferred_element_type=F32)
        out.append(part.astype(BF16))
    return jnp.concatenate(out, axis=1)


def terms(ids, days, ranks, penalties):
    dates = ids.shape[0]
    apart = jnp.abs(days - 196)
    season = jnp.minimum(apart, 365 - apart)
    bonus = jnp.where(ids == 1, 300, jnp.where(ids == 2, 500, 0))
    fixed = (16 * ranks + bonus - 4 * season) * dates + jnp.arange(dates, dtype=I32)
    return jnp.concatenate([fixed, penalties * dates]).astype(F32)


def fetches(source, target, sems, cuts):
    copies = [pltpu.make_async_copy(source.at[src], target.at[dst], sems.at[i]) for i, (src, dst) in enumerate(cuts)]
    for copy in copies:
        copy.start()
    return copies


def edge_kernel(words, first, last, near, sems):
    dates, rows, _ = words.shape
    row, col = iotas((dates * RADIUS, dates * TILE))
    whole = slice(None)
    cuts = [((whole, pl.ds(start, TILE)), side) for side, start in enumerate((0, rows - TILE))]
    copies = fetches(words, near, sems, cuts)
    for side, (out, shift) in enumerate(((first, 0), (last, TILE - RADIUS))):
        wanted = (row // RADIUS) * TILE + row % RADIUS + shift
        pick = (wanted == col).astype(F32).astype(BF16)
        copies[side].wait()
        level = obstruction(near[side]).reshape(dates * TILE, -1).astype(BF16)
        edge = jnp.dot(pick, level, preferred_element_type=F32).astype(BF16)
        out[...] = column_pass(edge)


def inner_kernel(scenes, words, keys, edge, near, sems):
    dates, rows, cols = words.shape
    copies = fetches(words, near, sems, [(pl.ds(t, GROUP), pl.ds(t, GROUP)) for t in range(0, dates, GROUP)])
    m, k = iotas((GROUP * rows, GROUP * rows))
    mix = jnp.where(m // rows == k // rows, tent(k % rows - m % rows), 0).astype(F32).astype(BF16)
    for step, copy in enumerate(copies):
        copy.wait()
        level = obstruction(near[step * GROUP : (step + 1) * GROUP]).reshape(GROUP * rows, cols).astype(BF16)
        across = column_pass(level)
        closeness = jnp.dot(mix, across, preferred_element_type=F32)
        best = None
        for i in range(GROUP):
            t = step * GROUP + i
            own = closeness[i * rows : (i + 1) * rows]
            edge[t, 0] = own[:TILE]
            edge[t, 1] = own[rows - TILE :]
            base, slope = scenes[t], scenes[dates + t]
            key = base - slope * own
            best = key if best is None else jnp.maximum(best, key)
        keys[...] = best if step == 0 else jnp.maximum(keys[...], best)


def small(value):
    return value.astype(F32).astype(BF16)


def coded(number):
    power = jnp.full(number.shape, 2.0**-64, F32)
    for bit in range(7):
        power = power * jnp.where(number & (1 << (7 + bit)) != 0, 2.0 ** (1 << bit), 1.0)
    return (((number & 127) + 128).astype(F32) * power).astype(BF16)


def pick_kernel(own, core, scenes, keys, edge, above, below, reflect, keep, send, cross, away, near, when, high, low, sems):
    dates, bands, rows, cols = reflect.shape
    across = cols // (2 * LANES)
    tall = keep.shape[2]
    whole = slice(None)
    cuts = [(whole, whole, pl.ds(row, tall)) for row in range(0, rows, tall)]
    copies = fetches(reflect, near, sems, [(cut, cut) for cut in cuts])
    parity = own[0] & 1
    m, k = iotas((dates * TILE, dates * RADIUS))
    same = m // TILE == k // RADIUS
    pairs = [(scenes[t], scenes[dates + t]) for t in range(dates)]
    ends = []
    for side, halo, shift in ((0, above, -RADIUS), (1, below, TILE)):
        mix = jnp.where(same, tent(k % RADIUS + shift - m % TILE), 0).astype(F32).astype(BF16)
        rest = jnp.dot(mix, halo[...], preferred_element_type=F32)
        best = None
        for t, (base, slope) in enumerate(pairs):
            key = base - slope * (edge[t, side] + rest[t * TILE : (t + 1) * TILE])
            best = key if best is None else jnp.maximum(best, key)
        ends.append(best)
    full = jnp.concatenate([ends[0], keys[TILE : rows - TILE], ends[1]], axis=0).astype(I32)
    full = full + FLOOR * dates
    date = full & (dates - 1)
    score = (full - date) // dates
    when[...] = small(date)
    high[...] = coded(score >> 3)
    low[...] = small((score & 7) * (2 * dates) + (parity * dates + date))
    for i, copy in enumerate(copies):
        copy.wait()
        for j in range(across // 2):
            slot = i * (across // 2) + j
            for side, half, out in ((1, 1, away), (1, 0, send), (0, 1, cross), (0, 0, keep)):
                col = pl.multiple_of((4 * j + 2 * (parity ^ side) + (core[0] ^ half)) * LANES, LANES)
                at = (pl.ds(i * tall, tall), pl.ds(col, LANES))
                chosen = when[at]
                hits = [chosen == jnp.asarray(t, BF16) for t in range(dates)]
                for band in range(bands):
                    value = near[(0, band, *at)]
                    for t in range(1, dates):
                        value = jnp.where(hits[t], near[(t, band, *at)], value)
                    out[slot, band] = value
                if half == 0:
                    out[slot, bands] = high[at]
                    out[slot, bands + 1] = low[at]


def pair_kernel(mine, mine_rest, other, other_rest, out):
    slots, groups = mine.shape[:2]
    bands = groups - 2
    for s in range(slots):
        high, low = mine[s, bands], mine[s, bands + 1]
        h, l = other[s, bands], other[s, bands + 1]
        better = (h > high) | ((h == high) & (l > low))
        for k in range(groups):
            out[s, k if k < bands else k + bands] = jnp.where(better, other[s, k], mine[s, k])
        for k in range(bands):
            out[s, bands + k] = jnp.where(better, other_rest[s, k], mine_rest[s, k])


def scored(low, dates):
    number = low.astype(F32).astype(I32)
    return small(number - (number & (dates - 1)))


def merge_kernel(dates, arrived, out):
    sources, groups = arrived.shape[:2]
    bands = groups - 2
    high, low = arrived[0, bands], arrived[0, bands + 1]
    floor = scored(low, dates)
    source = jnp.zeros(high.shape, BF16)
    values = [arrived[0, k] for k in range(bands)]
    for s in range(1, sources):
        h, l = arrived[s, bands], arrived[s, bands + 1]
        better = (h > high) | ((h == high) & (l >= floor))
        high, low = jnp.where(better, h, high), jnp.where(better, l, low)
        floor = jnp.where(better, scored(l, dates), floor)
        source = jnp.where(better, jnp.asarray(s, BF16), source)
        values = [jnp.where(better, arrived[s, k], v) for k, v in enumerate(values)]
    when = low.astype(F32).astype(I32) & (dates - 1)
    date = source.astype(F32) * dates + when.astype(F32)
    parts = [*values, date.astype(BF16)]
    for d in range(sources):
        for k, part in enumerate(parts):
            out[d, k] = part


def spread_kernel(own, core, mine, swapped, crossed, away, composite, best):
    slots, groups, tall, wide = mine.shape
    bands = composite.shape[0]
    across = best.shape[1] // (2 * wide)
    even, first = (own[0] & 1) == 0, core[0] == 0
    for owner in range(2 * slots):
        s = owner // 2
        here = even if owner % 2 == 0 else jnp.logical_not(even)
        rows = slice((owner // across) * tall, (owner // across + 1) * tall)
        for half in range(2):
            start = ((owner % across) * 2 + half) * wide
            cols = slice(start, start + wide)
            ours = first if half == 0 else jnp.logical_not(first)
            for k in range(bands + 1):
                near, far = (k, bands + k) if k < bands else (groups - 1, groups - 1)
                part = jnp.where(
                    ours,
                    jnp.where(here, mine[s, near], swapped[s, near]),
                    jnp.where(here, crossed[s, far], away[s, far]),
                )
                if k < bands:
                    composite[k, rows, cols] = part
                else:
                    best[rows, cols] = part.astype(F32).astype(I32)


def per_device(reflect, quality, instrument_ids, day_of_year, image_rank_values, cloud_penalty):
    dates, rows, cols = quality.shape
    bands = reflect.shape[1]
    sources, chips = lax.axis_size("date"), lax.axis_size("row")
    own, core = (lax.axis_index(a).astype(I32)[None] for a in ("date", "band"))
    across = cols // (2 * LANES)
    down = sources // across
    tall = rows // down
    shape = jax.ShapeDtypeStruct
    smem = pl.BlockSpec(memory_space=pltpu.SMEM)
    vmem = pl.BlockSpec(memory_space=pltpu.VMEM)
    hbm = pl.BlockSpec(memory_space=pltpu.HBM)
    scenes = terms(instrument_ids, day_of_year, image_rank_values, cloud_penalty)

    def grant(mib):
        return pltpu.CompilerParams(vmem_limit_bytes=mib << 20)

    row_shape = shape((dates * RADIUS, cols), BF16)
    first, last = pl.pallas_call(
        edge_kernel,
        out_shape=(row_shape, row_shape),
        in_specs=[hbm],
        out_specs=(vmem, vmem),
        scratch_shapes=[pltpu.VMEM((2, dates, TILE, cols), I32), pltpu.SemaphoreType.DMA((2,))],
        compiler_params=grant(BIG),
        name="edge",
    )(quality)
    onward = [(x, x + 1) for x in range(chips - 1)]
    above = lax.ppermute(last, "row", onward)
    below = lax.ppermute(first, "row", [(j, i) for i, j in onward])

    inner_keys, edge_part = pl.pallas_call(
        inner_kernel,
        out_shape=(shape((rows, cols), F32), shape((dates, 2, TILE, cols), F32)),
        in_specs=[smem, hbm],
        out_specs=(vmem, vmem),
        scratch_shapes=[pltpu.VMEM((dates, rows, cols), I32), pltpu.SemaphoreType.DMA((dates // GROUP,))],
        compiler_params=grant(BIG),
        name="inner",
    )(scenes, quality)

    slots = sources // 2

    def packed(groups):
        return shape((slots, groups, tall, LANES), BF16)

    plane = pltpu.VMEM((rows, cols), BF16)
    keep, send, cross, away = pl.pallas_call(
        pick_kernel,
        out_shape=(packed(bands + 2), packed(bands + 2), packed(bands), packed(bands)),
        in_specs=[smem] * 3 + [vmem] * 4 + [hbm],
        out_specs=(vmem,) * 4,
        scratch_shapes=[
            pltpu.VMEM((dates, bands, rows, cols), BF16), plane, plane, plane, pltpu.SemaphoreType.DMA((down,))
        ],
        compiler_params=grant(BIG),
        name="pick",
    )(own, core, scenes, inner_keys, edge_part, above, below, reflect)
    swap = [(z, z ^ 1) for z in range(sources)]
    diagonal = [(2 * z + c, 2 * (z ^ 1) + 1 - c) for z in range(sources) for c in range(2)]
    alike = [list(range(first, sources, 2)) for first in range(2)]

    def moved(parts, axes, pairs):
        return lax.ppermute(parts.reshape(-1, LANES), axes, pairs).reshape(parts.shape)

    def to_pair(parts):
        return moved(parts, "date", swap)

    def to_core(parts):
        return moved(parts, "band", [(0, 1), (1, 0)])

    def spread_out(parts):
        flat = parts.reshape(parts.shape[0], -1, LANES)
        return lax.all_to_all(flat, "date", 0, 0, axis_index_groups=alike, tiled=True).reshape(parts.shape)

    other, other_rest, mine_rest = to_pair(send), moved(away, ("date", "band"), diagonal), to_core(cross)
    paired = pl.pallas_call(
        pair_kernel,
        out_shape=packed(2 * bands + 2),
        in_specs=[vmem] * 4,
        out_specs=vmem,
        compiler_params=grant(8),
        name="pair",
    )(keep, mine_rest, other, other_rest)
    part = pl.pallas_call(
        functools.partial(merge_kernel, 2 * dates),
        out_shape=packed(2 * bands + 1),
        in_specs=[vmem],
        out_specs=vmem,
        compiler_params=grant(8),
        name="merge",
    )(spread_out(paired))
    parts = spread_out(part)
    beside = to_pair(parts)
    return pl.pallas_call(
        spread_kernel,
        out_shape=(shape((bands, rows, cols), BF16), shape((rows, cols), I32)),
        in_specs=[smem] * 2 + [vmem] * 4,
        out_specs=(vmem, vmem),
        compiler_params=grant(8),
        name="spread",
    )(own, core, parts, beside, to_core(parts), to_core(beside))


def solution(mesh):
    placed = (
        P("date", "band", ("grp", "row"), None),
        P("date", ("grp", "row"), None),
        P(("grp", "date")),
        P(("grp", "date")),
        P(("grp", "date")),
        P(("grp", "date")),
    )
    return jax.shard_map(
        per_device,
        mesh=mesh,
        in_specs=placed,
        out_specs=(P("band", ("grp", "row"), None), P(("grp", "row"), None)),
        check_vma=False,
    )
```

```python
import functools

import jax
import jax.numpy as jnp
from jax import lax
from jax.experimental import pallas as pl
from jax.experimental.pallas import tpu as pltpu
from jax.sharding import PartitionSpec as P

RADIUS = 4
TILE = 8
GROUP = 4
BLOCK = 256
LANES = 128
FLOOR = 126 * 1024
BIG = 50
F32 = jnp.float32
BF16 = jnp.bfloat16
I32 = jnp.int32


def tent(distance):
    return jnp.maximum(RADIUS + 1 - jnp.abs(distance), 0)


def iotas(shape):
    return lax.broadcasted_iota(I32, shape, 0), lax.broadcasted_iota(I32, shape, 1)


def obstruction(words):
    level = ((words >> 8) & 3) + ((words >> 10) & 3)
    return level.astype(F32)


def column_pass(blocked):
    cols = blocked.shape[1]
    side = BLOCK // 2
    k, n = iotas((2 * BLOCK, BLOCK))
    band = tent(k - side - n).astype(F32).astype(BF16)
    out = []
    for start in range(0, cols, BLOCK):
        low = max(0, start - side)
        high = min(cols, start + BLOCK + side)
        first = low - (start - side)
        part = jnp.dot(blocked[:, low:high], band[first : first + high - low], preferred_element_type=F32)
        out.append(part.astype(BF16))
    return jnp.concatenate(out, axis=1)


def terms(ids, days, ranks, penalties):
    dates = ids.shape[0]
    apart = jnp.abs(days - 196)
    season = jnp.minimum(apart, 365 - apart)
    bonus = jnp.where(ids == 1, 300, jnp.where(ids == 2, 500, 0))
    fixed = (16 * ranks + bonus - 4 * season) * dates + jnp.arange(dates, dtype=I32)
    return fixed, penalties * dates


def fetches(source, target, sems, cuts):
    copies = [pltpu.make_async_copy(source.at[src], target.at[dst], sems.at[i]) for i, (src, dst) in enumerate(cuts)]
    for copy in copies:
        copy.start()
    return copies


def edge_kernel(words, first, last, near, sems):
    dates, rows, _ = words.shape
    row, col = iotas((dates * RADIUS, dates * TILE))
    whole = slice(None)
    cuts = [((whole, pl.ds(start, TILE)), side) for side, start in enumerate((0, rows - TILE))]
    copies = fetches(words, near, sems, cuts)
    for side, (out, shift) in enumerate(((first, 0), (last, TILE - RADIUS))):
        wanted = (row // RADIUS) * TILE + row % RADIUS + shift
        pick = (wanted == col).astype(F32).astype(BF16)
        copies[side].wait()
        level = obstruction(near[side]).reshape(dates * TILE, -1).astype(BF16)
        edge = jnp.dot(pick, level, preferred_element_type=F32).astype(BF16)
        out[...] = column_pass(edge)


def inner_kernel(bases, slopes, words, keys, edge, near, sems):
    dates, rows, cols = words.shape
    copies = fetches(words, near, sems, [(pl.ds(t, GROUP), pl.ds(t, GROUP)) for t in range(0, dates, GROUP)])
    m, k = iotas((GROUP * rows, GROUP * rows))
    mix = jnp.where(m // rows == k // rows, tent(k % rows - m % rows), 0).astype(F32).astype(BF16)
    for step, copy in enumerate(copies):
        copy.wait()
        level = obstruction(near[step * GROUP : (step + 1) * GROUP]).reshape(GROUP * rows, cols).astype(BF16)
        across = column_pass(level)
        closeness = jnp.dot(mix, across, preferred_element_type=F32)
        best = None
        for i in range(GROUP):
            t = step * GROUP + i
            own = closeness[i * rows : (i + 1) * rows]
            edge[t, 0] = own[:TILE]
            edge[t, 1] = own[rows - TILE :]
            base, slope = bases[t].astype(F32), slopes[t].astype(F32)
            key = base - slope * own
            best = key if best is None else jnp.maximum(best, key)
        keys[...] = best if step == 0 else jnp.maximum(keys[...], best)


def small(value):
    return value.astype(F32).astype(BF16)


def coded(number):
    power = jnp.full(number.shape, 2.0**-64, F32)
    for bit in range(7):
        power = power * jnp.where(number & (1 << (7 + bit)) != 0, 2.0 ** (1 << bit), 1.0)
    return (((number & 127) + 128).astype(F32) * power).astype(BF16)


def blocks(reflect, near, sems, parity):
    across, whole = near.shape[3] // BLOCK, slice(None)
    tall = reflect.shape[2] * across // sems.shape[0]
    cuts = []
    for i in range(sems.shape[0] // across):
        for j in range(across):
            rows, col = pl.ds(i * tall, tall), pl.multiple_of((2 * j + parity) * BLOCK, BLOCK)
            cuts.append(((whole, whole, rows, pl.ds(col, BLOCK)), (whole, whole, rows, pl.ds(j * BLOCK, BLOCK))))
    return fetches(reflect, near, sems, cuts)


def choose(copies, near, parity, core, codes, coded_out, rest):
    dates, bands = near.shape[:2]
    tall = rest.shape[2]
    across = near.shape[3] // BLOCK
    for slot, copy in enumerate(copies):
        copy.wait()
        i, j = slot // across, slot % across
        rows = pl.ds(i * tall, tall)
        for half, out in enumerate((coded_out, rest)):
            lane = core ^ half
            at = (rows, pl.ds(pl.multiple_of((4 * j + 2 * parity + lane) * LANES, LANES), LANES))
            here = (rows, pl.ds(pl.multiple_of((2 * j + lane) * LANES, LANES), LANES))
            when, high, low = (code[at] for code in codes)
            hits = [when == jnp.asarray(t, BF16) for t in range(dates)]
            for band in range(bands):
                value = near[(0, band, *here)]
                for t in range(1, dates):
                    value = jnp.where(hits[t], near[(t, band, *here)], value)
                out[slot, band] = value
            if half == 0:
                out[slot, bands], out[slot, bands + 1] = high, low


def first_kernel(own, core, bases, slopes, keys, edge, above, below, reflect, send, away, when, high, low, near, sems):
    dates = reflect.shape[0]
    rows = keys.shape[0]
    parity = own[0] & 1
    copies = blocks(reflect, near, sems, parity ^ 1)
    m, k = iotas((dates * TILE, dates * RADIUS))
    same = m // TILE == k // RADIUS
    pairs = [(bases[t].astype(F32), slopes[t].astype(F32)) for t in range(dates)]
    ends = []
    for side, halo, shift in ((0, above, -RADIUS), (1, below, TILE)):
        mix = jnp.where(same, tent(k % RADIUS + shift - m % TILE), 0).astype(F32).astype(BF16)
        rest = jnp.dot(mix, halo[...], preferred_element_type=F32)
        best = None
        for t, (base, slope) in enumerate(pairs):
            key = base - slope * (edge[t, side] + rest[t * TILE : (t + 1) * TILE])
            best = key if best is None else jnp.maximum(best, key)
        ends.append(best)
    full = jnp.concatenate([ends[0], keys[TILE : rows - TILE], ends[1]], axis=0).astype(I32)
    full = full + FLOOR * dates
    date = full & (dates - 1)
    score = (full - date) // dates
    when[...] = small(date)
    high[...] = coded(score >> 3)
    low[...] = small((score & 7) * (2 * dates) + (parity * dates + date))
    choose(copies, near, parity ^ 1, core[0], (when, high, low), send, away)


def second_kernel(own, core, when, high, low, reflect, keep, cross, near, sems):
    parity = own[0] & 1
    copies = blocks(reflect, near, sems, parity)
    choose(copies, near, parity, core[0], (when, high, low), keep, cross)


def pair_kernel(mine, mine_rest, other, other_rest, out):
    slots, groups = mine.shape[:2]
    bands = groups - 2
    for s in range(slots):
        high, low = mine[s, bands], mine[s, bands + 1]
        h, l = other[s, bands], other[s, bands + 1]
        better = (h > high) | ((h == high) & (l > low))
        for k in range(groups):
            out[s, k if k < bands else k + bands] = jnp.where(better, other[s, k], mine[s, k])
        for k in range(bands):
            out[s, bands + k] = jnp.where(better, other_rest[s, k], mine_rest[s, k])


def scored(low, dates):
    number = low.astype(F32).astype(I32)
    return small(number - (number & (dates - 1)))


def merge_kernel(dates, arrived, out):
    sources, groups = arrived.shape[:2]
    bands = groups - 2
    high, low = arrived[0, bands], arrived[0, bands + 1]
    floor = scored(low, dates)
    source = jnp.zeros(high.shape, BF16)
    values = [arrived[0, k] for k in range(bands)]
    for s in range(1, sources):
        h, l = arrived[s, bands], arrived[s, bands + 1]
        better = (h > high) | ((h == high) & (l >= floor))
        high, low = jnp.where(better, h, high), jnp.where(better, l, low)
        floor = jnp.where(better, scored(l, dates), floor)
        source = jnp.where(better, jnp.asarray(s, BF16), source)
        values = [jnp.where(better, arrived[s, k], v) for k, v in enumerate(values)]
    when = low.astype(F32).astype(I32) & (dates - 1)
    date = source.astype(F32) * dates + when.astype(F32)
    parts = [*values, date.astype(BF16)]
    for d in range(sources):
        for k, part in enumerate(parts):
            out[d, k] = part


def spread_kernel(own, core, mine, swapped, crossed, away, composite, best):
    slots, groups, tall, wide = mine.shape
    bands = composite.shape[0]
    across = best.shape[1] // (2 * wide)
    even, first = (own[0] & 1) == 0, core[0] == 0
    for owner in range(2 * slots):
        s = owner // 2
        here = even if owner % 2 == 0 else jnp.logical_not(even)
        rows = slice((owner // across) * tall, (owner // across + 1) * tall)
        for half in range(2):
            start = ((owner % across) * 2 + half) * wide
            cols = slice(start, start + wide)
            ours = first if half == 0 else jnp.logical_not(first)
            for k in range(bands + 1):
                near, far = (k, bands + k) if k < bands else (groups - 1, groups - 1)
                part = jnp.where(
                    ours,
                    jnp.where(here, mine[s, near], swapped[s, near]),
                    jnp.where(here, crossed[s, far], away[s, far]),
                )
                if k < bands:
                    composite[k, rows, cols] = part
                else:
                    best[rows, cols] = part.astype(F32).astype(I32)


def per_device(reflect, quality, instrument_ids, day_of_year, image_rank_values, cloud_penalty):
    dates, rows, cols = quality.shape
    bands = reflect.shape[1]
    sources, chips = lax.axis_size("date"), lax.axis_size("row")
    own, core = (lax.axis_index(a).astype(I32)[None] for a in ("date", "band"))
    across = cols // (2 * LANES)
    down = sources // across
    tall = rows // down
    shape = jax.ShapeDtypeStruct
    smem = pl.BlockSpec(memory_space=pltpu.SMEM)
    vmem = pl.BlockSpec(memory_space=pltpu.VMEM)
    hbm = pl.BlockSpec(memory_space=pltpu.HBM)
    scenes = terms(instrument_ids, day_of_year, image_rank_values, cloud_penalty)

    def grant(mib):
        return pltpu.CompilerParams(vmem_limit_bytes=mib << 20)

    row_shape = shape((dates * RADIUS, cols), BF16)
    first, last = pl.pallas_call(
        edge_kernel,
        out_shape=(row_shape, row_shape),
        in_specs=[hbm],
        out_specs=(vmem, vmem),
        scratch_shapes=[pltpu.VMEM((2, dates, TILE, cols), I32), pltpu.SemaphoreType.DMA((2,))],
        compiler_params=grant(BIG),
        name="edge",
    )(quality)
    onward = [(x, x + 1) for x in range(chips - 1)]
    above = lax.ppermute(last, "row", onward)
    below = lax.ppermute(first, "row", [(j, i) for i, j in onward])

    inner_keys, edge_part = pl.pallas_call(
        inner_kernel,
        out_shape=(shape((rows, cols), F32), shape((dates, 2, TILE, cols), F32)),
        in_specs=[smem] * 2 + [hbm],
        out_specs=(vmem, vmem),
        scratch_shapes=[pltpu.VMEM((dates, rows, cols), I32), pltpu.SemaphoreType.DMA((dates // GROUP,))],
        compiler_params=grant(BIG),
        name="inner",
    )(*scenes, quality)

    slots = sources // 2

    def packed(groups):
        return shape((slots, groups, tall, LANES), BF16)

    plane = shape((rows, cols), BF16)
    scratch = [pltpu.VMEM((dates, bands, rows, cols // 2), BF16), pltpu.SemaphoreType.DMA((slots,))]
    send, away, *codes = pl.pallas_call(
        first_kernel,
        out_shape=(packed(bands + 2), packed(bands), plane, plane, plane),
        in_specs=[smem] * 4 + [vmem] * 4 + [hbm],
        out_specs=(vmem,) * 5,
        scratch_shapes=scratch,
        compiler_params=grant(BIG),
        name="first",
    )(own, core, *scenes, inner_keys, edge_part, above, below, reflect)
    keep, cross = pl.pallas_call(
        second_kernel,
        out_shape=(packed(bands + 2), packed(bands)),
        in_specs=[smem] * 2 + [vmem] * 3 + [hbm],
        out_specs=(vmem, vmem),
        scratch_shapes=scratch,
        compiler_params=grant(BIG),
        name="second",
    )(own, core, *codes, reflect)
    swap = [(z, z ^ 1) for z in range(sources)]
    diagonal = [(2 * z + c, 2 * (z ^ 1) + 1 - c) for z in range(sources) for c in range(2)]
    alike = [list(range(first, sources, 2)) for first in range(2)]

    def moved(parts, axes, pairs):
        return lax.ppermute(parts.reshape(-1, LANES), axes, pairs).reshape(parts.shape)

    def to_pair(parts):
        return moved(parts, "date", swap)

    def to_core(parts):
        return moved(parts, "band", [(0, 1), (1, 0)])

    def spread_out(parts):
        flat = parts.reshape(parts.shape[0], -1, LANES)
        return lax.all_to_all(flat, "date", 0, 0, axis_index_groups=alike, tiled=True).reshape(parts.shape)

    other, other_rest, mine_rest = to_pair(send), moved(away, ("date", "band"), diagonal), to_core(cross)
    paired = pl.pallas_call(
        pair_kernel,
        out_shape=packed(2 * bands + 2),
        in_specs=[vmem] * 4,
        out_specs=vmem,
        compiler_params=grant(8),
        name="pair",
    )(keep, mine_rest, other, other_rest)
    part = pl.pallas_call(
        functools.partial(merge_kernel, 2 * dates),
        out_shape=packed(2 * bands + 1),
        in_specs=[vmem],
        out_specs=vmem,
        compiler_params=grant(8),
        name="merge",
    )(spread_out(paired))
    parts = spread_out(part)
    beside = to_pair(parts)
    return pl.pallas_call(
        spread_kernel,
        out_shape=(shape((bands, rows, cols), BF16), shape((rows, cols), I32)),
        in_specs=[smem] * 2 + [vmem] * 4,
        out_specs=(vmem, vmem),
        compiler_params=grant(8),
        name="spread",
    )(own, core, parts, beside, to_core(parts), to_core(beside))


def solution(mesh):
    placed = (
        P("date", "band", ("grp", "row"), None),
        P("date", ("grp", "row"), None),
        P(("grp", "date")),
        P(("grp", "date")),
        P(("grp", "date")),
        P(("grp", "date")),
    )
    return jax.shard_map(
        per_device,
        mesh=mesh,
        in_specs=placed,
        out_specs=(P("band", ("grp", "row"), None), P(("grp", "row"), None)),
        check_vma=False,
    )
```

```python
import functools

import jax
import jax.numpy as jnp
from jax import lax
from jax.experimental import pallas as pl
from jax.experimental.pallas import tpu as pltpu
from jax.sharding import PartitionSpec as P

RADIUS = 4
TILE = 8
GROUP = 4
BLOCK = 256
LANES = 128
FLOOR = 126 * 1024
BIG = 50
F32 = jnp.float32
BF16 = jnp.bfloat16
I32 = jnp.int32


def tent(distance):
    return jnp.maximum(RADIUS + 1 - jnp.abs(distance), 0)


def iotas(shape):
    return lax.broadcasted_iota(I32, shape, 0), lax.broadcasted_iota(I32, shape, 1)


def obstruction(words):
    pair = (words >> 8) & 15
    return ((pair & 3) + (pair >> 2)).astype(F32)


def column_pass(blocked):
    cols = blocked.shape[1]
    side = BLOCK // 2
    k, n = iotas((2 * BLOCK, BLOCK))
    band = tent(k - side - n).astype(F32).astype(BF16)
    out = []
    for start in range(0, cols, BLOCK):
        low = max(0, start - side)
        high = min(cols, start + BLOCK + side)
        first = low - (start - side)
        part = jnp.dot(blocked[:, low:high], band[first : first + high - low], preferred_element_type=F32)
        out.append(part.astype(BF16))
    return jnp.concatenate(out, axis=1)


def terms(ids, days, ranks, penalties):
    dates = ids.shape[0]
    apart = jnp.abs(days - 196)
    season = jnp.minimum(apart, 365 - apart)
    bonus = jnp.where(ids == 1, 300, jnp.where(ids == 2, 500, 0))
    fixed = (16 * ranks + bonus - 4 * season) * dates + jnp.arange(dates, dtype=I32)
    return fixed, penalties * dates


def fetches(source, target, sems, cuts):
    copies = [pltpu.make_async_copy(source.at[src], target.at[dst], sems.at[i]) for i, (src, dst) in enumerate(cuts)]
    for copy in copies:
        copy.start()
    return copies


def edge_kernel(words, first, last, near, sems):
    dates, rows, _ = words.shape
    whole = slice(None)
    cuts = [((whole, pl.ds(start, TILE)), side) for side, start in enumerate((0, rows - TILE))]
    copies = fetches(words, near, sems, cuts)
    sent = dates * RADIUS
    row, col = iotas((2 * sent, 2 * dates * TILE))
    wanted = (row // RADIUS) * TILE + row % RADIUS + (row // sent) * (TILE - RADIUS)
    pick = (wanted == col).astype(F32).astype(BF16)
    for copy in copies:
        copy.wait()
    level = obstruction(near[...]).reshape(2 * dates * TILE, -1).astype(BF16)
    edge = jnp.dot(pick, level, preferred_element_type=F32).astype(BF16)
    across = column_pass(edge)
    first[...] = across[:sent]
    last[...] = across[sent:]


def inner_kernel(bases, slopes, words, keys, edge, near, sems):
    dates, rows, cols = words.shape
    copies = fetches(words, near, sems, [(pl.ds(t, GROUP), pl.ds(t, GROUP)) for t in range(0, dates, GROUP)])
    m, k = iotas((GROUP * rows, GROUP * rows))
    mix = jnp.where(m // rows == k // rows, tent(k % rows - m % rows), 0).astype(F32).astype(BF16)
    for step, copy in enumerate(copies):
        copy.wait()
        level = obstruction(near[step * GROUP : (step + 1) * GROUP]).reshape(GROUP * rows, cols).astype(BF16)
        across = column_pass(level)
        closeness = jnp.dot(mix, across, preferred_element_type=F32)
        best = None
        for i in range(GROUP):
            t = step * GROUP + i
            own = closeness[i * rows : (i + 1) * rows]
            edge[t, 0] = own[:TILE]
            edge[t, 1] = own[rows - TILE :]
            base, slope = bases[t].astype(F32), slopes[t].astype(F32)
            key = base - slope * own
            best = key if best is None else jnp.maximum(best, key)
        keys[...] = best if step == 0 else jnp.maximum(keys[...], best)


def small(value):
    return value.astype(F32).astype(BF16)


def coded(number):
    power = jnp.full(number.shape, 2.0**-64, F32)
    for bit in range(7):
        power = power * jnp.where(number & (1 << (7 + bit)) != 0, 2.0 ** (1 << bit), 1.0)
    return (((number & 127) + 128).astype(F32) * power).astype(BF16)


def blocks(reflect, near, sems, parity):
    across, whole = near.shape[3] // BLOCK, slice(None)
    tall = reflect.shape[2] * across // sems.shape[0]
    cuts = []
    for i in range(sems.shape[0] // across):
        for j in range(across):
            rows, col = pl.ds(i * tall, tall), pl.multiple_of((2 * j + parity) * BLOCK, BLOCK)
            cuts.append(((whole, whole, rows, pl.ds(col, BLOCK)), (whole, whole, rows, pl.ds(j * BLOCK, BLOCK))))
    return fetches(reflect, near, sems, cuts)


def choose(copies, near, parity, core, codes, coded_out, rest):
    dates, bands = near.shape[:2]
    tall = rest.shape[2]
    across = near.shape[3] // BLOCK
    for slot, copy in enumerate(copies):
        copy.wait()
        i, j = slot // across, slot % across
        rows = pl.ds(i * tall, tall)
        for half, out in enumerate((coded_out, rest)):
            lane = core ^ half
            at = (rows, pl.ds(pl.multiple_of((4 * j + 2 * parity + lane) * LANES, LANES), LANES))
            here = (rows, pl.ds(pl.multiple_of((2 * j + lane) * LANES, LANES), LANES))
            when, high, low = (code[at] for code in codes)
            hits = [when == jnp.asarray(t, BF16) for t in range(dates)]
            for band in range(bands):
                value = near[(0, band, *here)]
                for t in range(1, dates):
                    value = jnp.where(hits[t], near[(t, band, *here)], value)
                out[slot, band] = value
            if half == 0:
                out[slot, bands], out[slot, bands + 1] = high, low


def first_kernel(own, core, bases, slopes, keys, edge, above, below, reflect, send, away, when, high, low, near, sems):
    dates = reflect.shape[0]
    rows = keys.shape[0]
    parity = own[0] & 1
    copies = blocks(reflect, near, sems, parity ^ 1)
    m, k = iotas((dates * TILE, dates * RADIUS))
    same = m // TILE == k // RADIUS
    pairs = [(bases[t].astype(F32), slopes[t].astype(F32)) for t in range(dates)]
    ends = []
    for side, halo, shift in ((0, above, -RADIUS), (1, below, TILE)):
        mix = jnp.where(same, tent(k % RADIUS + shift - m % TILE), 0).astype(F32).astype(BF16)
        rest = jnp.dot(mix, halo[...], preferred_element_type=F32)
        best = None
        for t, (base, slope) in enumerate(pairs):
            key = base - slope * (edge[t, side] + rest[t * TILE : (t + 1) * TILE])
            best = key if best is None else jnp.maximum(best, key)
        ends.append(best)
    full = jnp.concatenate([ends[0], keys[TILE : rows - TILE], ends[1]], axis=0).astype(I32)
    full = full + FLOOR * dates
    date = full & (dates - 1)
    score = (full - date) // dates
    when[...] = small(date)
    high[...] = coded(score >> 3)
    low[...] = small((score & 7) * (2 * dates) + (parity * dates + date))
    choose(copies, near, parity ^ 1, core[0], (when, high, low), send, away)


def second_kernel(own, core, when, high, low, reflect, keep, cross, near, sems):
    parity = own[0] & 1
    copies = blocks(reflect, near, sems, parity)
    choose(copies, near, parity, core[0], (when, high, low), keep, cross)


def pair_kernel(mine, mine_rest, other, other_rest, out):
    slots, groups = mine.shape[:2]
    bands = groups - 2
    for s in range(slots):
        high, low = mine[s, bands], mine[s, bands + 1]
        h, l = other[s, bands], other[s, bands + 1]
        better = (h > high) | ((h == high) & (l > low))
        for k in range(groups):
            out[s, k if k < bands else k + bands] = jnp.where(better, other[s, k], mine[s, k])
        for k in range(bands):
            out[s, bands + k] = jnp.where(better, other_rest[s, k], mine_rest[s, k])


def scored(low, dates):
    number = low.astype(F32).astype(I32)
    return small(number - (number & (dates - 1)))


def merge_kernel(dates, arrived, out):
    sources, groups = arrived.shape[:2]
    bands = groups - 2
    high, low = arrived[0, bands], arrived[0, bands + 1]
    floor = scored(low, dates)
    source = jnp.zeros(high.shape, BF16)
    values = [arrived[0, k] for k in range(bands)]
    for s in range(1, sources):
        h, l = arrived[s, bands], arrived[s, bands + 1]
        better = (h > high) | ((h == high) & (l >= floor))
        high, low = jnp.where(better, h, high), jnp.where(better, l, low)
        floor = jnp.where(better, scored(l, dates), floor)
        source = jnp.where(better, jnp.asarray(s, BF16), source)
        values = [jnp.where(better, arrived[s, k], v) for k, v in enumerate(values)]
    when = low.astype(F32).astype(I32) & (dates - 1)
    date = source.astype(F32) * dates + when.astype(F32)
    parts = [*values, date.astype(BF16)]
    for d in range(sources):
        for k, part in enumerate(parts):
            out[d, k] = part


def spread_kernel(own, core, mine, swapped, crossed, away, composite, best):
    slots, groups, tall, wide = mine.shape
    bands = composite.shape[0]
    across = best.shape[1] // (2 * wide)
    even, first = (own[0] & 1) == 0, core[0] == 0
    for owner in range(2 * slots):
        s = owner // 2
        here = even if owner % 2 == 0 else jnp.logical_not(even)
        rows = slice((owner // across) * tall, (owner // across + 1) * tall)
        for half in range(2):
            start = ((owner % across) * 2 + half) * wide
            cols = slice(start, start + wide)
            ours = first if half == 0 else jnp.logical_not(first)
            for k in range(bands + 1):
                near, far = (k, bands + k) if k < bands else (groups - 1, groups - 1)
                part = jnp.where(
                    ours,
                    jnp.where(here, mine[s, near], swapped[s, near]),
                    jnp.where(here, crossed[s, far], away[s, far]),
                )
                if k < bands:
                    composite[k, rows, cols] = part
                else:
                    best[rows, cols] = part.astype(F32).astype(I32)


def per_device(reflect, quality, instrument_ids, day_of_year, image_rank_values, cloud_penalty):
    dates, rows, cols = quality.shape
    bands = reflect.shape[1]
    sources, chips = lax.axis_size("date"), lax.axis_size("row")
    own, core = (lax.axis_index(a).astype(I32)[None] for a in ("date", "band"))
    across = cols // (2 * LANES)
    down = sources // across
    tall = rows // down
    shape = jax.ShapeDtypeStruct
    smem = pl.BlockSpec(memory_space=pltpu.SMEM)
    vmem = pl.BlockSpec(memory_space=pltpu.VMEM)
    hbm = pl.BlockSpec(memory_space=pltpu.HBM)
    scenes = terms(instrument_ids, day_of_year, image_rank_values, cloud_penalty)

    def grant(mib):
        return pltpu.CompilerParams(vmem_limit_bytes=mib << 20)

    row_shape = shape((dates * RADIUS, cols), BF16)
    first, last = pl.pallas_call(
        edge_kernel,
        out_shape=(row_shape, row_shape),
        in_specs=[hbm],
        out_specs=(vmem, vmem),
        scratch_shapes=[pltpu.VMEM((2, dates, TILE, cols), I32), pltpu.SemaphoreType.DMA((2,))],
        compiler_params=grant(BIG),
        name="edge",
    )(quality)
    onward = [(x, x + 1) for x in range(chips - 1)]
    above = lax.ppermute(last, "row", onward)
    below = lax.ppermute(first, "row", [(j, i) for i, j in onward])

    inner_keys, edge_part = pl.pallas_call(
        inner_kernel,
        out_shape=(shape((rows, cols), F32), shape((dates, 2, TILE, cols), F32)),
        in_specs=[smem] * 2 + [hbm],
        out_specs=(vmem, vmem),
        scratch_shapes=[pltpu.VMEM((dates, rows, cols), I32), pltpu.SemaphoreType.DMA((dates // GROUP,))],
        compiler_params=grant(BIG),
        name="inner",
    )(*scenes, quality)

    slots = sources // 2

    def packed(groups):
        return shape((slots, groups, tall, LANES), BF16)

    plane = shape((rows, cols), BF16)
    scratch = [pltpu.VMEM((dates, bands, rows, cols // 2), BF16), pltpu.SemaphoreType.DMA((slots,))]
    send, away, *codes = pl.pallas_call(
        first_kernel,
        out_shape=(packed(bands + 2), packed(bands), plane, plane, plane),
        in_specs=[smem] * 4 + [vmem] * 4 + [hbm],
        out_specs=(vmem,) * 5,
        scratch_shapes=scratch,
        compiler_params=grant(BIG),
        name="first",
    )(own, core, *scenes, inner_keys, edge_part, above, below, reflect)
    keep, cross = pl.pallas_call(
        second_kernel,
        out_shape=(packed(bands + 2), packed(bands)),
        in_specs=[smem] * 2 + [vmem] * 3 + [hbm],
        out_specs=(vmem, vmem),
        scratch_shapes=scratch,
        compiler_params=grant(BIG),
        name="second",
    )(own, core, *codes, reflect)
    swap = [(z, z ^ 1) for z in range(sources)]
    diagonal = [(2 * z + c, 2 * (z ^ 1) + 1 - c) for z in range(sources) for c in range(2)]
    alike = [list(range(first, sources, 2)) for first in range(2)]

    def moved(parts, axes, pairs):
        return lax.ppermute(parts.reshape(-1, LANES), axes, pairs).reshape(parts.shape)

    def to_pair(parts):
        return moved(parts, "date", swap)

    def to_core(parts):
        return moved(parts, "band", [(0, 1), (1, 0)])

    def spread_out(parts):
        flat = parts.reshape(parts.shape[0], -1, LANES)
        return lax.all_to_all(flat, "date", 0, 0, axis_index_groups=alike, tiled=True).reshape(parts.shape)

    other, other_rest, mine_rest = to_pair(send), moved(away, ("date", "band"), diagonal), to_core(cross)
    paired = pl.pallas_call(
        pair_kernel,
        out_shape=packed(2 * bands + 2),
        in_specs=[vmem] * 4,
        out_specs=vmem,
        compiler_params=grant(8),
        name="pair",
    )(keep, mine_rest, other, other_rest)
    part = pl.pallas_call(
        functools.partial(merge_kernel, 2 * dates),
        out_shape=packed(2 * bands + 1),
        in_specs=[vmem],
        out_specs=vmem,
        compiler_params=grant(8),
        name="merge",
    )(spread_out(paired))
    parts = spread_out(part)
    beside = to_pair(parts)
    return pl.pallas_call(
        spread_kernel,
        out_shape=(shape((bands, rows, cols), BF16), shape((rows, cols), I32)),
        in_specs=[smem] * 2 + [vmem] * 4,
        out_specs=(vmem, vmem),
        compiler_params=grant(8),
        name="spread",
    )(own, core, parts, beside, to_core(parts), to_core(beside))


def solution(mesh):
    placed = (
        P("date", "band", ("grp", "row"), None),
        P("date", ("grp", "row"), None),
        P(("grp", "date")),
        P(("grp", "date")),
        P(("grp", "date")),
        P(("grp", "date")),
    )
    return jax.shard_map(
        per_device,
        mesh=mesh,
        in_specs=placed,
        out_specs=(P("band", ("grp", "row"), None), P(("grp", "row"), None)),
        check_vma=False,
    )
```
